32 devices in a mesh: groups: 2 (over y), ffn: 4 (over z), hidden: 4 (over x, core).
Axes of the slice: x: 2, y: 2, z: 4, core: 2. Of those that a mesh axis runs over, the one named last changes fastest.
Arguments:
- residual_in: bfloat16 [512, 8192], P(('groups', 'ffn'), 'hidden'), parts along dimension 0, may hold values from -10 to 10
- queries: bfloat16 [512, 8192], P(('groups', 'hidden'), 'ffn'), parts along dimension 0, may hold values from -100 to 100
- new_keys: bfloat16 [512, 1024], P(('groups', 'hidden'), 'ffn'), parts along dimension 0, may hold values from -6 to 6
- new_values: bfloat16 [512, 1024], P(('groups', 'hidden'), 'ffn'), parts along dimension 0, may hold values from -24 to 24
- key_cache: bfloat16 [32, 2048, 1024], P(('groups', 'hidden'), 'ffn'), parts along dimension 0, may hold values from -6 to 6
- value_cache: bfloat16 [32, 2048, 1024], P(('groups', 'hidden'), 'ffn'), parts along dimension 0, may hold values from -24 to 24
- cache_lengths: int32 [32], P(('groups', 'hidden')), parts along dimension 0, may hold values from 1 to 2048, as said below
- norm_gain: bfloat16 [8192], P('hidden'), may hold values from 0.099609375 to 1.8984375
- out_weight: bfloat16 [8192, 8192], P('ffn', 'hidden'), may hold values from -0.25 to 0.25
- gate_weight: bfloat16 [8192, 14336], P('hidden', 'ffn'), may hold values from -0.125 to 0.125
- up_weight: bfloat16 [8192, 14336], P('hidden', 'ffn'), may hold values from -0.125 to 0.125
- down_weight: bfloat16 [14336, 8192], P('ffn', 'hidden'), may hold values from -0.09375 to 0.09375
Outputs:
- block_out: bfloat16 [512, 8192], P(('groups', 'ffn'), 'hidden'), parts along dimension 0
The draws below stay inside these ranges and needn't reach their ends.
There are 2 independent parts, one for each index of `groups`. The reference program is written for one: setup_inputs(seed, part) draws one part's arguments, and reference() takes and returns one part's arrays. A program takes and returns all parts, laid end to end along the dimension named above; an argument that names none is the same for every part. Nothing has to cross between parts.
Inputs may be any that keep to these rules, and one draw needn't show every extreme that they name: `cache_lengths`: each sequence's cached tokens fill the first cache positions; some sequence has exactly 2048.
All inputs are finite; a program needn't handle non-finite values.
Results may differ from the reference program's by a relative error of at most 0.04.
Values may be sent and summed in bfloat16 or wider, within the bound.
A program may use at most 128 MiB of HBM per device.

```python
import math
import jax
import jax.numpy as jnp
from jax import lax

D = 8192
HEADS = 64
KVH = 8
HD = 128
FF = 14336
DRAFT = 16
CTX = 2048
SEQS = 16
ROWS = 256
N_FFN = 4
N_HIDDEN = 4


def draw_residual_in(key, part):
    ramp = 0.6 + 1.4 * jnp.arange(D).astype(jnp.float32) / D
    base = jnp.clip(jax.random.normal(key, (ROWS, D), jnp.float32), -5.0, 5.0)
    return (base * ramp[None, :]).astype(jnp.bfloat16)


def draw_queries(key, part):
    base = jnp.clip(jax.random.normal(key, (ROWS, HEADS * HD), jnp.float32), -4.0, 4.0)
    return base.astype(jnp.bfloat16)


def draw_cache_lengths(key, part):
    first_key, second_key = jax.random.split(jax.random.fold_in(key, 3))
    drawn = jax.random.randint(first_key, (SEQS,), 1, CTX + 1)
    chosen_seq = jax.random.randint(second_key, (), 0, SEQS)
    return jnp.where(jnp.arange(SEQS) == chosen_seq, CTX, drawn).astype(jnp.int32)


def level_of(key, extent, cuts, least, top_value):
    def one(dim, blocks):
        draws = jax.random.uniform(jax.random.fold_in(jax.random.fold_in(key, 6), dim), (blocks,), jnp.float32, least / len(cuts), top_value / len(cuts))
        return jnp.repeat(jnp.exp(draws), extent[dim] // blocks).reshape((-1,) + (1,) * (len(extent) - dim - 1))

    gain = one(*cuts[0])
    for cut in cuts[1:]:
        gain = gain * one(*cut)
    return gain


def gaussian(own_key, extent, deviation, limit, shards=(), kind=jnp.bfloat16):
    entries = jax.random.normal(own_key, extent, jnp.float32) * deviation
    if len(shards) > 0:
        entries = level_of(own_key, extent, shards, -0.22, 0.18) * entries
    return jnp.clip(entries, min=-limit, max=limit).astype(kind)


def setup_inputs(seed: int = 0, part: int = 0) -> dict:
    key_of = jax.random.split(jax.random.key(seed), 13)
    part_splits = jax.random.split(jax.random.fold_in(key_of[12], part), 13)
    return {
        "residual_in": draw_residual_in(jax.random.fold_in(jax.random.fold_in(key_of[12], part), 71), part),
        "queries": draw_queries(jax.random.fold_in(jax.random.fold_in(key_of[12], part), 71), part),
        "new_keys": gaussian(part_splits[2], (ROWS, KVH * HD), 1.0, 6.0, ((0, 4), (1, 4))),
        "new_values": gaussian(part_splits[3], (ROWS, KVH * HD), 4.0, 24.0, ((0, 4), (1, 4))),
        "key_cache": gaussian(part_splits[4], (SEQS, CTX, KVH * HD), 1.0, 6.0, ((0, 4), (1, 4))),
        "value_cache": gaussian(part_splits[5], (SEQS, CTX, KVH * HD), 4.0, 24.0, ((0, 4), (1, 4))),
        "cache_lengths": draw_cache_lengths(jax.random.fold_in(jax.random.fold_in(key_of[12], part), 71), part),
        "norm_gain": jnp.clip(1.0 + 0.18 * jax.random.normal(key_of[7], (D,), jnp.float32), 0.099609375, 1.8984375).astype(jnp.bfloat16),
        "out_weight": gaussian(key_of[8], (HEADS * HD, D), (HEADS * HD // 16) ** -0.5, 0.25, ((0, 4), (1, 4))),
        "gate_weight": gaussian(key_of[9], (D, FF), (D // 4) ** -0.5, 0.125, ((0, 4), (1, 4))),
        "up_weight": gaussian(key_of[10], (D, FF), (D // 4) ** -0.5, 0.125, ((0, 4), (1, 4))),
        "down_weight": gaussian(key_of[11], (FF, D), (FF // 4) ** -0.5, 0.09375, ((0, 4), (1, 4))),
    }


def rope_tables(positions):
    steps_half = jnp.arange(HD // 2).astype(jnp.float32)
    inverse = jnp.exp(steps_half * (-2.0 * math.log(500000.0) / HD))
    angle = positions.astype(jnp.float32)[:, None] * inverse[None, :]
    return (jnp.cos(angle), jnp.sin(angle))

def rotate(values, cosine, sine_table):
    half = values.shape[-1] // 2
    first_half = values[..., :half]
    second_half = values[..., half:]
    cosine = cosine[:, None, :]
    sine_table = sine_table[:, None, :]
    return jnp.concatenate([first_half * cosine - second_half * sine_table, second_half * cosine + first_half * sine_table], axis=-1)

def rounded(values):
    return lax.optimization_barrier(values.astype(jnp.bfloat16)).astype(jnp.float32)

def one_sequence(inputs):
    queries, new_keys, new_values, key_cache, value_cache, length = inputs
    group = HEADS // KVH
    block = CTX // N_FFN
    positions = length + jnp.arange(DRAFT, dtype=jnp.int32)
    cosine, sine_table = rope_tables(positions)
    query_rot = rounded(rotate(queries.astype(jnp.float32).reshape(DRAFT, HEADS, HD), cosine, sine_table))
    query_rot = query_rot.reshape(DRAFT, KVH, group, HD)
    key_rot = rounded(rotate(new_keys.astype(jnp.float32).reshape(DRAFT, KVH, HD), cosine, sine_table))
    cached_keys = key_cache.astype(jnp.float32).reshape(CTX, KVH, HD)
    scaling = 1.0 / math.sqrt(HD)
    cache_scores = jnp.einsum('jkgd,pkd->jkgp', query_rot, cached_keys) * scaling
    draft_scores = jnp.einsum('jkgd,ikd->jkgi', query_rot, key_rot) * scaling
    usable = jnp.arange(CTX) < length
    causal = (jnp.arange(DRAFT)[None, :] <= jnp.arange(DRAFT)[:, None])[:, None, None, :]
    cache_scores = jnp.where(usable, cache_scores, -1e+30)
    draft_scores = jnp.where(causal, draft_scores, -1e+30)
    peak_score = jnp.maximum(cache_scores.max(-1), draft_scores.max(-1))[..., None]
    cache_weights = jnp.where(usable, jnp.exp(cache_scores - peak_score), 0.0)
    draft_weights = jnp.where(causal, jnp.exp(draft_scores - peak_score), 0.0)
    cached_values = value_cache.astype(jnp.float32).reshape(N_FFN, block, KVH, HD)
    block_weights = cache_weights.reshape(DRAFT, KVH, group, N_FFN, block)
    numerator = jnp.einsum('jkgbp,bpkd->bjkgd', rounded(block_weights), cached_values)
    denominator = jnp.moveaxis(block_weights.sum(-1), -1, 0)
    draft_values = new_values.astype(jnp.float32).reshape(DRAFT, KVH, HD)
    numerator = numerator.at[0].add(jnp.einsum('jkgi,ikd->jkgd', rounded(draft_weights), draft_values))
    denominator = denominator.at[0].add(draft_weights.sum(-1))
    numerator = lax.optimization_barrier(jnp.sum(rounded(numerator), axis=0))
    denominator = lax.optimization_barrier(jnp.sum(rounded(denominator), axis=0))
    return (numerator / denominator[..., None]).reshape(DRAFT, HEADS * HD).astype(jnp.bfloat16)

def blockwise(left, right, pieces):
    width = left.shape[1] // pieces

    def add_piece(counter, total):
        offset = (counter * width).astype(jnp.int32)
        left_part = lax.dynamic_slice_in_dim(left, offset, width, 1)
        right_part = lax.dynamic_slice_in_dim(right, offset, width, 0)
        return total + rounded(jnp.dot(left_part, right_part, preferred_element_type=jnp.float32))
    initial = jnp.zeros((left.shape[0], right.shape[1]), jnp.float32)
    return lax.fori_loop(0, pieces, add_piece, initial)

def reference(residual_in, queries, new_keys, new_values, key_cache, value_cache, cache_lengths, norm_gain, out_weight, gate_weight, up_weight, down_weight):
    attended = lax.map(one_sequence, (queries.reshape(SEQS, DRAFT, HEADS * HD), new_keys.reshape(SEQS, DRAFT, KVH * HD), new_values.reshape(SEQS, DRAFT, KVH * HD), key_cache, value_cache, cache_lengths))
    attended = attended.reshape(ROWS, HEADS * HD)
    projected = blockwise(attended, out_weight, N_FFN)
    resid = (residual_in.astype(jnp.float32) + projected).astype(jnp.bfloat16)
    widened = resid.astype(jnp.float32)
    factor = lax.rsqrt(lax.optimization_barrier(jnp.mean(widened * widened, axis=1, keepdims=True)) + 1e-05)
    normed = (widened * factor * norm_gain.astype(jnp.float32)[None, :]).astype(jnp.bfloat16)
    gate = blockwise(normed, gate_weight, N_HIDDEN)
    upward = blockwise(normed, up_weight, N_HIDDEN)
    activation = (jax.nn.silu(gate) * upward).astype(jnp.bfloat16)
    lowered = blockwise(activation, down_weight, N_FFN)
    return (widened + lowered).astype(jnp.bfloat16)
```

```python
import functools
import math

import jax
import jax.numpy as jnp
from jax import lax
from jax.experimental import pallas as pl
from jax.experimental.pallas import tpu as pltpu
from jax.sharding import PartitionSpec as P

D = 8192
HEADS = 64
KVH = 8
HD = 128
DRAFT = 16
GROUP = HEADS // KVH
F32 = jnp.float32
BF16 = jnp.bfloat16
MESH = pl.DeviceIdType.MESH
SLOTS = 3


def kernel(
    cfg,
    cos_ref,
    sin_ref,
    bias_ref,
    dbias_ref,
    q_ref,
    k_ref,
    v_ref,
    resin_ref,
    gain_ref,
    kc_hbm,
    vc_hbm,
    ow_hbm,
    gw_hbm,
    uw_hbm,
    dw_hbm,
    out_ref,
    kbuf,
    vbuf,
    ow,
    gbuf,
    ubuf,
    dw,
    qall,
    kall,
    vall,
    num_send,
    num_recv,
    lse_send,
    lse_recv,
    att,
    pp,
    pp_recv,
    resid,
    sq,
    sq_recv,
    nrm,
    part,
    r1,
    s2,
    s2_recv,
    act,
    acc,
    dn_recv,
    kv_sem,
    w_sem,
    gu_sem,
    qkv_ss,
    qkv_rs,
    num_ss,
    num_rs,
    att_ss,
    att_rs,
    pp_ss,
    pp_rs,
    sq_ss,
    sq_rs,
    nrm_ss,
    nrm_rs,
    r1_ss,
    r1_rs,
    s2_ss,
    s2_rs,
    act_ss,
    act_rs,
    dn_ss,
    dn_rs,
):
    nf, nh, seqs, tile, tiles = cfg
    nx = nh // 2
    me_f = lax.axis_index("ffn")
    me_h = lax.axis_index("hidden")
    core = lax.rem(me_h, 2)
    me_x = me_h // 2
    partner = me_x * 2 + (1 - core)
    rows = q_ref.shape[0]
    rr = resin_ref.shape[0]
    width = resin_ref.shape[1]
    hh = q_ref.shape[1] // HD

    def fpeer(d):
        return lax.rem(me_f + d, nf)

    def ffrom(d):
        return lax.rem(me_f + nf - d, nf)

    def hpeer(d):
        return lax.rem(me_h + d, nh)

    def xpeer(d):
        return lax.rem(me_x + d, nx) * 2 + core

    def xfrom(d):
        return lax.rem(me_x + nx - d, nx)

    def fcopy(src, dst, ss, rs, dev):
        return pltpu.make_async_remote_copy(
            src_ref=src, dst_ref=dst, send_sem=ss, recv_sem=rs,
            device_id={"ffn": dev}, device_id_type=MESH,
        )

    def hcopy(src, dst, ss, rs, dev):
        return pltpu.make_async_remote_copy(
            src_ref=src, dst_ref=dst, send_sem=ss, recv_sem=rs,
            device_id={"hidden": dev}, device_id_type=MESH,
        )

    def kv_copies(s):
        slot = lax.rem(s, 2)
        return (
            pltpu.make_async_copy(kc_hbm.at[s], kbuf.at[slot], kv_sem.at[0, slot]),
            pltpu.make_async_copy(vc_hbm.at[s], vbuf.at[slot], kv_sem.at[1, slot]),
        )

    def gu_copies(t):
        slot = lax.rem(t, SLOTS)
        if tiles == 1:
            cols = pl.ds(0, tile)
        else:
            cols = pl.ds(pl.multiple_of(t * tile, tile), tile)
        return (
            pltpu.make_async_copy(gw_hbm.at[:, cols], gbuf.at[slot], gu_sem.at[0, slot]),
            pltpu.make_async_copy(uw_hbm.at[:, cols], ubuf.at[slot], gu_sem.at[1, slot]),
        )

    ow_copy = pltpu.make_async_copy(ow_hbm, ow, w_sem.at[0])
    dw_copy = pltpu.make_async_copy(dw_hbm, dw, w_sem.at[1])

    for s in range(min(2, seqs)):
        for c in kv_copies(s):
            c.start()

    barrier = pltpu.get_barrier_semaphore()
    for d in range(1, nf):
        pl.semaphore_signal(barrier, inc=1, device_id={"ffn": fpeer(d)}, device_id_type=MESH)
    for d in range(1, nh):
        pl.semaphore_signal(barrier, inc=1, device_id={"hidden": hpeer(d)}, device_id_type=MESH)

    cos = cos_ref[...]
    sin = sin_ref[...]

    for h in range(hh):
        x = q_ref[:, h * HD : (h + 1) * HD].astype(F32)
        qall[me_f, :, h * HD : (h + 1) * HD] = (
            x * cos + pltpu.roll(x, HD // 2, 1) * sin
        ).astype(BF16)
    kall[me_f] = k_ref[...]
    vall[me_f] = v_ref[...]

    pl.semaphore_wait(barrier, nf - 1 + nh - 1)

    def qkv(d):
        return [
            fcopy(buf.at[me_f], buf.at[me_f], qkv_ss.at[i, d], qkv_rs.at[i, d], fpeer(d))
            for i, buf in enumerate((qall, kall, vall))
        ]

    for d in range(1, nf):
        for c in qkv(d):
            c.start()
    ow_copy.start()
    for d in range(1, nf):
        for c in qkv(d):
            c.wait_recv()

    kw = k_ref.shape[1]

    def kv_head(buf, k, r0):
        if kw >= HD:
            per = kw // HD
            lo = (k % per) * HD
            return buf[k // per, pl.ds(r0, DRAFT), lo : lo + HD]
        per = HD // kw
        return jnp.concatenate(
            [buf[k * per + i, pl.ds(r0, DRAFT), :] for i in range(per)], axis=1
        )

    scaling = 1.0 / math.sqrt(HD)
    nt = (((1,), (1,)), ((), ()))

    def attend(s, carry):
        slot = lax.rem(s, 2)
        for c in kv_copies(s):
            c.wait()
        r0 = pl.multiple_of(s * DRAFT, DRAFT)
        cs = cos_ref[pl.ds(r0, DRAFT), :]
        sn = sin_ref[pl.ds(r0, DRAFT), :]
        bias = bias_ref[s]
        dbias = dbias_ref[...]
        for k in range(KVH):
            pieces = []
            for g in range(GROUP):
                h = k * GROUP + g
                lo = (h % hh) * HD
                pieces.append(qall[h // hh, pl.ds(r0, DRAFT), lo : lo + HD])
            q = jnp.concatenate(pieces, axis=0)
            keys = kbuf[slot, :, k * HD : (k + 1) * HD]
            values = vbuf[slot, :, k * HD : (k + 1) * HD]
            kd = kv_head(kall, k, r0).astype(F32)
            kd = (kd * cs + pltpu.roll(kd, HD // 2, 1) * sn).astype(BF16)
            vd = kv_head(vall, k, r0)
            sc = lax.dot_general(q, keys, nt, preferred_element_type=F32) * scaling + bias
            sd = lax.dot_general(q, kd, nt, preferred_element_type=F32) * scaling + dbias
            m = jnp.maximum(
                jnp.max(sc, axis=1, keepdims=True), jnp.max(sd, axis=1, keepdims=True)
            )
            w = jnp.exp(sc - m)
            wd = jnp.exp(sd - m)
            total = jnp.sum(w, axis=1, keepdims=True) + jnp.sum(wd, axis=1, keepdims=True)
            num = jnp.dot(w.astype(BF16), values, preferred_element_type=F32)
            num = num + jnp.dot(wd.astype(BF16), vd, preferred_element_type=F32)
            o = (num / total).astype(BF16)
            lse = m + jnp.log(total)
            for g in range(GROUP):
                h = k * GROUP + g
                lo = (h % hh) * HD
                num_send[h // hh, pl.ds(r0, DRAFT), lo : lo + HD] = o[
                    g * DRAFT : (g + 1) * DRAFT
                ]
                lse_send[h // hh, pl.ds(r0, DRAFT), h % hh : h % hh + 1] = lse[
                    g * DRAFT : (g + 1) * DRAFT
                ]

        @pl.when(s + 2 < seqs)
        def _():
            for c in kv_copies(s + 2):
                c.start()

        return carry

    lax.fori_loop(0, seqs, attend, 0)

    def nums(d):
        p = fpeer(d)
        return [
            fcopy(num_send.at[p], num_recv.at[d - 1], num_ss.at[0, d], num_rs.at[0, d], p),
            fcopy(lse_send.at[p], lse_recv.at[d - 1], num_ss.at[1, d], num_rs.at[1, d], p),
        ]

    for d in range(1, nf):
        for c in nums(d):
            c.start()
    for t in range(min(SLOTS, tiles)):
        for c in gu_copies(t):
            c.start()
    dw_copy.start()
    for d in range(1, nf):
        for c in nums(d):
            c.wait_recv()
    for h in range(hh):
        lo = h * HD
        ls = [lse_send[me_f, :, h : h + 1]] + [
            lse_recv[d - 1, :, h : h + 1] for d in range(1, nf)
        ]
        ns = [num_send[me_f, :, lo : lo + HD]] + [
            num_recv[d - 1, :, lo : lo + HD] for d in range(1, nf)
        ]
        top = functools.reduce(jnp.maximum, ls)
        ws = [jnp.exp(x - top) for x in ls]
        tot = functools.reduce(jnp.add, ws)
        val = functools.reduce(jnp.add, [w * n.astype(F32) for w, n in zip(ws, ns)])
        att[me_h, :, lo : lo + HD] = (val / tot).astype(BF16)

    def att_x(d):
        return hcopy(att.at[me_h], att.at[me_h], att_ss.at[d], att_rs.at[d], xpeer(d))

    def att_p(d):
        b = xfrom(d) * 2 + core
        return hcopy(att.at[b], att.at[b], att_ss.at[nx + d], att_rs.at[nx + d], partner)

    for d in range(1, nx):
        att_x(d).start()
    att_p(0).start()
    for d in range(1, nx):
        att_x(d).wait_recv()
        att_p(d).start()
    for d in range(nx):
        att_p(d).wait_recv()

    ow_copy.wait()
    step = width if width % 512 else 512
    total_rows = nh * rows

    def project(i, carry):
        cols = pl.ds(pl.multiple_of(i * step, step), step) if width != step else slice(None)
        x = att[...].reshape(total_rows, att.shape[2])
        pp[:, cols] = jnp.dot(x, ow[:, cols], preferred_element_type=F32).astype(BF16)
        return carry

    lax.fori_loop(0, width // step, project, 0)

    def own_rows(p):
        return pl.ds(pl.multiple_of(p * rr, rr), rr)

    def pps(d):
        p = fpeer(d)
        return fcopy(pp.at[own_rows(p)], pp_recv.at[d - 1], pp_ss.at[d], pp_rs.at[d], p)

    for d in range(1, nf):
        pps(d).start()
    for d in range(1, nf):
        pps(d).wait_recv()
    x = pp[own_rows(me_f), :].astype(F32)
    for d in range(1, nf):
        x = x + pp_recv[d - 1].astype(F32)
    x = (resin_ref[...].astype(F32) + x).astype(BF16).astype(F32)
    resid[...] = x
    mine = jnp.sum(x * x, axis=1, keepdims=True)
    sq[...] = jnp.broadcast_to(mine, sq.shape)

    def sqs(d):
        return hcopy(sq, sq_recv.at[d - 1], sq_ss.at[d], sq_rs.at[d], hpeer(d))

    for d in range(1, nh):
        sqs(d).start()
    for d in range(1, nh):
        sqs(d).wait_recv()
    squares = mine
    for d in range(1, nh):
        squares = squares + sq_recv[d - 1, :, 0:1]
    factor = lax.rsqrt(squares / D + 1e-05)
    nrm[me_f] = (resid[...] * factor * gain_ref[...].astype(F32)).astype(BF16)

    def nrms(d):
        return fcopy(nrm.at[me_f], nrm.at[me_f], nrm_ss.at[d], nrm_rs.at[d], fpeer(d))

    for d in range(1, nf):
        nrms(d).start()
    acc[...] = jnp.zeros_like(acc)
    dw_copy.wait()
    for d in range(1, nf):
        nrms(d).wait_recv()

    qr = total_rows // nh

    def r1_copy(t):
        return hcopy(part.at[t, 1 - core], r1.at[t], r1_ss.at[t], r1_rs.at[t], partner)

    def s2_copy(t, d):
        return hcopy(
            s2.at[t, d - 1], s2_recv.at[t, d - 1], s2_ss.at[t, d], s2_rs.at[t, d], xpeer(d)
        )

    def act_x(t, d):
        a = act.at[t, me_h]
        return hcopy(a, a, act_ss.at[t, d], act_rs.at[t, d], xpeer(d))

    def act_p(t, d):
        a = act.at[t, xfrom(d) * 2 + core]
        return hcopy(a, a, act_ss.at[t, nx + d], act_rs.at[t, nx + d], partner)

    def inner(t, carry):
        @pl.when(t < tiles)
        def _():
            slot = lax.rem(t, SLOTS)
            for c in gu_copies(t):
                c.wait()
            x = nrm[...].reshape(total_rows, width)
            for i, buf in enumerate((gbuf, ubuf)):
                y = jnp.dot(x, buf[slot], preferred_element_type=F32).astype(BF16)
                for b in range(nh):
                    part[t, b % 2, b // 2, i] = y[b * qr : (b + 1) * qr]
            r1_copy(t).start()

            @pl.when(t + SLOTS < tiles)
            def _():
                for c in gu_copies(t + SLOTS):
                    c.start()

        @pl.when(jnp.logical_and(t >= 1, t < tiles + 1))
        def _():
            u = t - 1
            r1_copy(u).wait_recv()
            for d in range(1, nx):
                o = lax.rem(me_x + d, nx)
                s2[u, d - 1] = (
                    part[u, core, o].astype(F32) + r1[u, o].astype(F32)
                ).astype(BF16)
                s2_copy(u, d).start()

        @pl.when(jnp.logical_and(t >= 2, t < tiles + 2))
        def _():
            u = t - 2
            for d in range(1, nx):
                s2_copy(u, d).wait_recv()
            y = part[u, core, me_x].astype(F32) + r1[u, me_x].astype(F32)
            for d in range(1, nx):
                y = y + s2_recv[u, d - 1].astype(F32)
            gate = y[0]
            up = y[1]
            act[u, me_h] = (gate / (1.0 + jnp.exp(-gate)) * up).astype(BF16)
            for d in range(1, nx):
                act_x(u, d).start()
            act_p(u, 0).start()

        @pl.when(jnp.logical_and(t >= 3, t < tiles + 3))
        def _():
            u = t - 3
            for d in range(1, nx):
                act_x(u, d).wait_recv()
                act_p(u, d).start()

        @pl.when(t >= 4)
        def _():
            u = t - 4
            for d in range(nx):
                act_p(u, d).wait_recv()
            x = act[u].reshape(total_rows, tile)
            k0 = pl.multiple_of(u * tile, tile)

            def down(i, c):
                cols = pl.ds(pl.multiple_of(i * step, step), step) if width != step else slice(None)
                acc[:, cols] += jnp.dot(x, dw[pl.ds(k0, tile), cols], preferred_element_type=F32)
                return c

            lax.fori_loop(0, width // step, down, 0)

        return carry

    lax.fori_loop(0, tiles + 4, inner, 0)

    for d in range(1, nf):
        pps(d).wait_send()
    pp[...] = acc[...].astype(BF16)

    def dns(d):
        p = fpeer(d)
        return fcopy(pp.at[own_rows(p)], dn_recv.at[d - 1], dn_ss.at[d], dn_rs.at[d], p)

    for d in range(1, nf):
        dns(d).start()
    for d in range(1, nf):
        dns(d).wait_recv()
    y = pp[own_rows(me_f), :].astype(F32)
    for d in range(1, nf):
        y = y + dn_recv[d - 1].astype(F32)
    out_ref[...] = (resid[...] + y).astype(BF16)

    for d in range(1, nf):
        for c in qkv(d) + nums(d):
            c.wait_send()
        nrms(d).wait_send()
        dns(d).wait_send()
    for d in range(1, nh):
        sqs(d).wait_send()
    for d in range(1, nx):
        att_x(d).wait_send()
    for d in range(nx):
        att_p(d).wait_send()

    def drain(t, carry):
        r1_copy(t).wait_send()
        for d in range(1, nx):
            s2_copy(t, d).wait_send()
            act_x(t, d).wait_send()
        for d in range(nx):
            act_p(t, d).wait_send()
        return carry

    lax.fori_loop(0, tiles, drain, 0)


def solution(mesh):
    nf = mesh.shape["ffn"]
    nh = mesh.shape["hidden"]
    nx = nh // 2

    def shards(
        residual_in, queries, new_keys, new_values, key_cache, value_cache,
        cache_lengths, norm_gain, out_weight, gate_weight, up_weight, down_weight,
    ):
        seqs, block, kvw = key_cache.shape
        rows, qw = queries.shape
        kw = new_keys.shape[1]
        rr, width = residual_in.shape
        units = gate_weight.shape[1]
        hh = qw // HD
        tile = 512 if units % 512 == 0 else units
        tiles = units // tile
        total_rows = rows * nh
        qr = total_rows // nh

        positions = cache_lengths[:, None] + jnp.arange(DRAFT, dtype=jnp.int32)[None, :]
        steps_half = jnp.arange(HD // 2).astype(F32)
        inverse = jnp.exp(steps_half * (-2.0 * math.log(500000.0) / HD))
        angle = positions.reshape(-1).astype(F32)[:, None] * inverse[None, :]
        cos, sin = jnp.cos(angle), jnp.sin(angle)
        cos = jnp.concatenate([cos, cos], axis=1)
        sin = jnp.concatenate([-sin, sin], axis=1)
        ffn = lax.axis_index("ffn")
        slots = ffn * block + jnp.arange(block, dtype=jnp.int32)
        bias = jnp.where(slots[None, :] < cache_lengths[:, None], 0.0, -1e30).astype(F32)
        bias = bias[:, None, :]
        token = jnp.arange(GROUP * DRAFT, dtype=jnp.int32) % DRAFT
        causal = jnp.arange(DRAFT, dtype=jnp.int32)[None, :] <= token[:, None]
        dbias = jnp.where(jnp.logical_and(causal, ffn == 0), 0.0, -1e30).astype(F32)

        vm = pl.BlockSpec(memory_space=pltpu.VMEM)
        hbm = pl.BlockSpec(memory_space=pl.ANY)
        dma = pltpu.SemaphoreType.DMA
        V = pltpu.VMEM
        scratch = [
            V((2, block, kvw), BF16),
            V((2, block, kvw), BF16),
            V(out_weight.shape, BF16),
            V((SLOTS, width, tile), BF16),
            V((SLOTS, width, tile), BF16),
            V(down_weight.shape, BF16),
            V((nf, rows, qw), BF16),
            V((nf, rows, kw), BF16),
            V((nf, rows, kw), BF16),
            V((nf, rows, qw), BF16),
            V((nf - 1, rows, qw), BF16),
            V((nf, rows, hh), F32),
            V((nf - 1, rows, hh), F32),
            V((nh, rows, qw), BF16),
            V((total_rows, width), BF16),
            V((nf - 1, rr, width), BF16),
            V((rr, width), F32),
            V((rr, HD), F32),
            V((nh - 1, rr, HD), F32),
            V((nf, rr, width), BF16),
            V((tiles, 2, nx, 2, qr, tile), BF16),
            V((tiles, nx, 2, qr, tile), BF16),
            V((tiles, nx - 1, 2, qr, tile), BF16),
            V((tiles, nx - 1, 2, qr, tile), BF16),
            V((tiles, nh, qr, tile), BF16),
            V((total_rows, width), F32),
            V((nf - 1, rr, width), BF16),
            dma((2, 2)),
            dma((2,)),
            dma((2, SLOTS)),
            dma((3, nf)), dma((3, nf)),
            dma((2, nf)), dma((2, nf)),
            dma((2 * nx,)), dma((2 * nx,)),
            dma((nf,)), dma((nf,)),
            dma((nh,)), dma((nh,)),
            dma((nf,)), dma((nf,)),
            dma((tiles,)), dma((tiles,)),
            dma((tiles, nx)), dma((tiles, nx)),
            dma((tiles, 2 * nx)), dma((tiles, 2 * nx)),
            dma((nf,)), dma((nf,)),
        ]
        return pl.pallas_call(
            functools.partial(kernel, (nf, nh, seqs, tile, tiles)),
            out_shape=jax.ShapeDtypeStruct((rr, width), BF16),
            in_specs=[vm] * 9 + [hbm] * 6,
            out_specs=vm,
            scratch_shapes=scratch,
            compiler_params=pltpu.CompilerParams(
                collective_id=0, has_side_effects=True, vmem_limit_bytes=67043328
            ),
        )(
            cos, sin, bias, dbias, queries, new_keys, new_values, residual_in,
            norm_gain[None, :], key_cache, value_cache, out_weight, gate_weight,
            up_weight, down_weight,
        )

    in_specs = (
        P(("groups", "ffn"), "hidden"),
        P(("groups", "hidden"), "ffn"),
        P(("groups", "hidden"), "ffn"),
        P(("groups", "hidden"), "ffn"),
        P(("groups", "hidden"), "ffn", None),
        P(("groups", "hidden"), "ffn", None),
        P(("groups", "hidden")),
        P("hidden"),
        P("ffn", "hidden"),
        P("hidden", "ffn"),
        P("hidden", "ffn"),
        P("ffn", "hidden"),
    )
    out_specs = P(("groups", "ffn"), "hidden")
    return jax.shard_map(shards, mesh=mesh, in_specs=in_specs, out_specs=out_specs, check_vma=False)
```

```python
import functools
import math

import jax
import jax.numpy as jnp
from jax import lax
from jax.experimental import pallas as pl
from jax.experimental.pallas import tpu as pltpu
from jax.sharding import PartitionSpec as P

D = 8192
HEADS = 64
KVH = 8
HD = 128
DRAFT = 16
GROUP = HEADS // KVH
F32 = jnp.float32
BF16 = jnp.bfloat16
MESH = pl.DeviceIdType.MESH
SLOTS = 3


def kernel(
    cfg,
    cos_ref,
    sin_ref,
    bias_ref,
    dbias_ref,
    q_ref,
    k_ref,
    v_ref,
    resin_ref,
    gain_ref,
    kc_hbm,
    vc_hbm,
    ow_hbm,
    gw_hbm,
    uw_hbm,
    dw_hbm,
    out_ref,
    kbuf,
    vbuf,
    ow,
    gbuf,
    ubuf,
    dw,
    qall,
    kall,
    vall,
    num_send,
    num_recv,
    lse_send,
    lse_recv,
    att,
    pp,
    pp_recv,
    resid,
    sq,
    sq_recv,
    nrm,
    part,
    r1,
    s2,
    s2_recv,
    act,
    acc,
    dn_recv,
    low,
    kv_sem,
    w_sem,
    gu_sem,
    qkv_ss,
    qkv_rs,
    num_ss,
    num_rs,
    att_ss,
    att_rs,
    pp_ss,
    pp_rs,
    sq_ss,
    sq_rs,
    nrm_ss,
    nrm_rs,
    r1_ss,
    r1_rs,
    s2_ss,
    s2_rs,
    act_ss,
    act_rs,
    dn_ss,
    dn_rs,
):
    nf, nh, seqs, tile, tiles = cfg
    nx = nh // 2
    me_f = lax.axis_index("ffn")
    me_h = lax.axis_index("hidden")
    core = lax.rem(me_h, 2)
    me_x = me_h // 2
    partner = me_x * 2 + (1 - core)
    rows = q_ref.shape[0]
    rr = resin_ref.shape[0]
    width = resin_ref.shape[1]
    hh = q_ref.shape[1] // HD

    def fpeer(d):
        return lax.rem(me_f + d, nf)

    def ffrom(d):
        return lax.rem(me_f + nf - d, nf)

    def hpeer(d):
        return lax.rem(me_h + d, nh)

    def xpeer(d):
        return lax.rem(me_x + d, nx) * 2 + core

    def xfrom(d):
        return lax.rem(me_x + nx - d, nx)

    def fcopy(src, dst, ss, rs, dev):
        return pltpu.make_async_remote_copy(
            src_ref=src, dst_ref=dst, send_sem=ss, recv_sem=rs,
            device_id={"ffn": dev}, device_id_type=MESH,
        )

    def hcopy(src, dst, ss, rs, dev):
        return pltpu.make_async_remote_copy(
            src_ref=src, dst_ref=dst, send_sem=ss, recv_sem=rs,
            device_id={"hidden": dev}, device_id_type=MESH,
        )

    has_left = me_f > 0
    has_right = me_f < nf - 1

    def g_copy(buf, ss, rs, i, right, b):
        return fcopy(
            buf.at[b], buf.at[b], ss.at[i, right, b], rs.at[i, b],
            me_f + 1 if right else me_f - 1,
        )

    def chain_start(bufs, ss, rs):
        for i, buf in enumerate(bufs):

            @pl.when(has_right)
            def _():
                g_copy(buf, ss, rs, i, 1, me_f).start()

            @pl.when(has_left)
            def _():
                g_copy(buf, ss, rs, i, 0, me_f).start()

    def chain_finish(bufs, ss, rs):
        for d in range(1, nf):
            for i, buf in enumerate(bufs):

                @pl.when(me_f >= d)
                def _():
                    g_copy(buf, ss, rs, i, 1, me_f - d).wait_recv()

                    @pl.when(has_right)
                    def _():
                        g_copy(buf, ss, rs, i, 1, me_f - d).start()

                @pl.when(me_f + d < nf)
                def _():
                    g_copy(buf, ss, rs, i, 0, me_f + d).wait_recv()

                    @pl.when(has_left)
                    def _():
                        g_copy(buf, ss, rs, i, 0, me_f + d).start()

    def chain_drain(bufs, ss, rs):
        for d in range(nf):
            for i, buf in enumerate(bufs):

                @pl.when(jnp.logical_and(me_f >= d, has_right))
                def _():
                    g_copy(buf, ss, rs, i, 1, me_f - d).wait_send()

                @pl.when(jnp.logical_and(me_f + d < nf, has_left))
                def _():
                    g_copy(buf, ss, rs, i, 0, me_f + d).wait_send()

    def r_copy(recv, ss, rs, right, o):
        return fcopy(
            pp.at[pl.ds(o * rr, rr)], recv.at[right, o], ss.at[o], rs.at[right, o],
            me_f + 1 if right else me_f - 1,
        )

    def chain_reduce(recv, ss, rs, total):
        for j in range(nf - 1):
            for right, o in ((1, nf - 1 - j), (0, j)):
                far = me_f < o if right else me_f > o
                feeds = has_left if right else has_right

                @pl.when(far)
                def _():
                    @pl.when(feeds)
                    def _():
                        r_copy(recv, ss, rs, right, o).wait_recv()
                        block = pl.ds(o * rr, rr)
                        pp[block, :] = (
                            pp[block, :].astype(F32) + recv[right, o].astype(F32)
                        ).astype(BF16)

                    r_copy(recv, ss, rs, right, o).start()

        total[...] = pp[own_rows(me_f), :].astype(F32)
        for right, feeds in ((1, has_left), (0, has_right)):

            @pl.when(feeds)
            def _():
                fcopy(
                    pp.at[own_rows(me_f)], recv.at[right, me_f], ss.at[me_f],
                    rs.at[right, me_f], me_f - 1 if right else me_f + 1,
                ).wait_recv()
                total[...] += recv[right, me_f].astype(F32)

    def reduce_drain(recv, ss, rs):
        for o in range(nf):

            @pl.when(me_f < o)
            def _():
                r_copy(recv, ss, rs, 1, o).wait_send()

            @pl.when(me_f > o)
            def _():
                r_copy(recv, ss, rs, 0, o).wait_send()

    def own_rows(p):
        return pl.ds(pl.multiple_of(p * rr, rr), rr)

    def kv_copies(s):
        slot = lax.rem(s, 2)
        return (
            pltpu.make_async_copy(kc_hbm.at[s], kbuf.at[slot], kv_sem.at[0, slot]),
            pltpu.make_async_copy(vc_hbm.at[s], vbuf.at[slot], kv_sem.at[1, slot]),
        )

    def gu_copies(t):
        slot = lax.rem(t, SLOTS)
        if tiles == 1:
            cols = pl.ds(0, tile)
        else:
            cols = pl.ds(pl.multiple_of(t * tile, tile), tile)
        return (
            pltpu.make_async_copy(gw_hbm.at[:, cols], gbuf.at[slot], gu_sem.at[0, slot]),
            pltpu.make_async_copy(uw_hbm.at[:, cols], ubuf.at[slot], gu_sem.at[1, slot]),
        )

    ow_copy = pltpu.make_async_copy(ow_hbm, ow, w_sem.at[0])
    dw_copy = pltpu.make_async_copy(dw_hbm, dw, w_sem.at[1])

    for s in range(min(2, seqs)):
        for c in kv_copies(s):
            c.start()

    barrier = pltpu.get_barrier_semaphore()
    for d in range(1, nf):
        pl.semaphore_signal(barrier, inc=1, device_id={"ffn": fpeer(d)}, device_id_type=MESH)
    for d in range(1, nh):
        pl.semaphore_signal(barrier, inc=1, device_id={"hidden": hpeer(d)}, device_id_type=MESH)

    cos = cos_ref[...]
    sin = sin_ref[...]

    for h in range(hh):
        x = q_ref[:, h * HD : (h + 1) * HD].astype(F32)
        qall[me_f, :, h * HD : (h + 1) * HD] = (
            x * cos + pltpu.roll(x, HD // 2, 1) * sin
        ).astype(BF16)
    kall[me_f] = k_ref[...]
    vall[me_f] = v_ref[...]

    pl.semaphore_wait(barrier, nf - 1 + nh - 1)

    chain_start((qall, kall, vall), qkv_ss, qkv_rs)
    ow_copy.start()
    chain_finish((qall, kall, vall), qkv_ss, qkv_rs)

    kw = k_ref.shape[1]

    def kv_head(buf, k, r0):
        if kw >= HD:
            per = kw // HD
            lo = (k % per) * HD
            return buf[k // per, pl.ds(r0, DRAFT), lo : lo + HD]
        per = HD // kw
        return jnp.concatenate(
            [buf[k * per + i, pl.ds(r0, DRAFT), :] for i in range(per)], axis=1
        )

    scaling = 1.0 / math.sqrt(HD)
    nt = (((1,), (1,)), ((), ()))

    def attend(s, carry):
        slot = lax.rem(s, 2)
        for c in kv_copies(s):
            c.wait()
        r0 = pl.multiple_of(s * DRAFT, DRAFT)
        cs = cos_ref[pl.ds(r0, DRAFT), :]
        sn = sin_ref[pl.ds(r0, DRAFT), :]
        bias = bias_ref[s]
        dbias = dbias_ref[...]
        for k in range(KVH):
            pieces = []
            for g in range(GROUP):
                h = k * GROUP + g
                lo = (h % hh) * HD
                pieces.append(qall[h // hh, pl.ds(r0, DRAFT), lo : lo + HD])
            q = jnp.concatenate(pieces, axis=0)
            keys = kbuf[slot, :, k * HD : (k + 1) * HD]
            values = vbuf[slot, :, k * HD : (k + 1) * HD]
            kd = kv_head(kall, k, r0).astype(F32)
            kd = (kd * cs + pltpu.roll(kd, HD // 2, 1) * sn).astype(BF16)
            vd = kv_head(vall, k, r0)
            sc = lax.dot_general(q, keys, nt, preferred_element_type=F32) * scaling + bias
            sd = lax.dot_general(q, kd, nt, preferred_element_type=F32) * scaling + dbias
            m = jnp.maximum(
                jnp.max(sc, axis=1, keepdims=True), jnp.max(sd, axis=1, keepdims=True)
            )
            w = jnp.exp(sc - m)
            wd = jnp.exp(sd - m)
            total = jnp.sum(w, axis=1, keepdims=True) + jnp.sum(wd, axis=1, keepdims=True)
            num = jnp.dot(w.astype(BF16), values, preferred_element_type=F32)
            num = num + jnp.dot(wd.astype(BF16), vd, preferred_element_type=F32)
            o = (num / total).astype(BF16)
            lse = m + jnp.log(total)
            for g in range(GROUP):
                h = k * GROUP + g
                lo = (h % hh) * HD
                num_send[h // hh, pl.ds(r0, DRAFT), lo : lo + HD] = o[
                    g * DRAFT : (g + 1) * DRAFT
                ]
                lse_send[h // hh, pl.ds(r0, DRAFT), h % hh : h % hh + 1] = lse[
                    g * DRAFT : (g + 1) * DRAFT
                ]

        @pl.when(s + 2 < seqs)
        def _():
            for c in kv_copies(s + 2):
                c.start()

        return carry

    lax.fori_loop(0, seqs, attend, 0)

    def nums(d):
        p = fpeer(d)
        return [
            fcopy(num_send.at[p], num_recv.at[d - 1], num_ss.at[0, d], num_rs.at[0, d], p),
            fcopy(lse_send.at[p], lse_recv.at[d - 1], num_ss.at[1, d], num_rs.at[1, d], p),
        ]

    for d in range(1, nf):
        for c in nums(d):
            c.start()
    for t in range(min(SLOTS, tiles)):
        for c in gu_copies(t):
            c.start()
    dw_copy.start()
    for d in range(1, nf):
        for c in nums(d):
            c.wait_recv()
    for h in range(hh):
        lo = h * HD
        ls = [lse_send[me_f, :, h : h + 1]] + [
            lse_recv[d - 1, :, h : h + 1] for d in range(1, nf)
        ]
        ns = [num_send[me_f, :, lo : lo + HD]] + [
            num_recv[d - 1, :, lo : lo + HD] for d in range(1, nf)
        ]
        top = functools.reduce(jnp.maximum, ls)
        ws = [jnp.exp(x - top) for x in ls]
        tot = functools.reduce(jnp.add, ws)
        val = functools.reduce(jnp.add, [w * n.astype(F32) for w, n in zip(ws, ns)])
        att[me_h, :, lo : lo + HD] = (val / tot).astype(BF16)

    def att_x(d):
        return hcopy(att.at[me_h], att.at[me_h], att_ss.at[d], att_rs.at[d], xpeer(d))

    def att_p(d):
        b = xfrom(d) * 2 + core
        return hcopy(att.at[b], att.at[b], att_ss.at[nx + d], att_rs.at[nx + d], partner)

    for d in range(1, nx):
        att_x(d).start()
    att_p(0).start()
    for d in range(1, nx):
        att_x(d).wait_recv()
        att_p(d).start()
    for d in range(nx):
        att_p(d).wait_recv()

    ow_copy.wait()
    step = width if width % 512 else 512
    total_rows = nh * rows

    def project(i, carry):
        cols = pl.ds(pl.multiple_of(i * step, step), step) if width != step else slice(None)
        x = att[...].reshape(total_rows, att.shape[2])
        pp[:, cols] = jnp.dot(x, ow[:, cols], preferred_element_type=F32).astype(BF16)
        return carry

    lax.fori_loop(0, width // step, project, 0)

    chain_reduce(pp_recv, pp_ss, pp_rs, resid)
    x = resid[...]
    x = (resin_ref[...].astype(F32) + x).astype(BF16).astype(F32)
    resid[...] = x
    mine = jnp.sum(x * x, axis=1, keepdims=True)
    sq[...] = jnp.broadcast_to(mine, sq.shape)

    def sqs(d):
        return hcopy(sq, sq_recv.at[d - 1], sq_ss.at[d], sq_rs.at[d], hpeer(d))

    for d in range(1, nh):
        sqs(d).start()
    for d in range(1, nh):
        sqs(d).wait_recv()
    squares = mine
    for d in range(1, nh):
        squares = squares + sq_recv[d - 1, :, 0:1]
    factor = lax.rsqrt(squares / D + 1e-05)
    nrm[me_f] = (resid[...] * factor * gain_ref[...].astype(F32)).astype(BF16)

    chain_start((nrm,), nrm_ss, nrm_rs)
    acc[...] = jnp.zeros_like(acc)
    dw_copy.wait()
    chain_finish((nrm,), nrm_ss, nrm_rs)

    qr = total_rows // nh

    def r1_copy(t):
        return hcopy(part.at[t, 1 - core], r1.at[t], r1_ss.at[t], r1_rs.at[t], partner)

    def s2_copy(t, d):
        return hcopy(
            s2.at[t, d - 1], s2_recv.at[t, d - 1], s2_ss.at[t, d], s2_rs.at[t, d], xpeer(d)
        )

    def act_x(t, d):
        a = act.at[t, me_h]
        return hcopy(a, a, act_ss.at[t, d], act_rs.at[t, d], xpeer(d))

    def act_p(t, d):
        a = act.at[t, xfrom(d) * 2 + core]
        return hcopy(a, a, act_ss.at[t, nx + d], act_rs.at[t, nx + d], partner)

    def inner(t, carry):
        @pl.when(t < tiles)
        def _():
            slot = lax.rem(t, SLOTS)
            for c in gu_copies(t):
                c.wait()
            x = nrm[...].reshape(total_rows, width)
            for i, buf in enumerate((gbuf, ubuf)):
                y = jnp.dot(x, buf[slot], preferred_element_type=F32).astype(BF16)
                for b in range(nh):
                    part[t, b % 2, b // 2, i] = y[b * qr : (b + 1) * qr]
            r1_copy(t).start()

            @pl.when(t + SLOTS < tiles)
            def _():
                for c in gu_copies(t + SLOTS):
                    c.start()

        @pl.when(jnp.logical_and(t >= 1, t < tiles + 1))
        def _():
            u = t - 1
            r1_copy(u).wait_recv()
            for d in range(1, nx):
                o = lax.rem(me_x + d, nx)
                s2[u, d - 1] = (
                    part[u, core, o].astype(F32) + r1[u, o].astype(F32)
                ).astype(BF16)
                s2_copy(u, d).start()

        @pl.when(jnp.logical_and(t >= 2, t < tiles + 2))
        def _():
            u = t - 2
            for d in range(1, nx):
                s2_copy(u, d).wait_recv()
            y = part[u, core, me_x].astype(F32) + r1[u, me_x].astype(F32)
            for d in range(1, nx):
                y = y + s2_recv[u, d - 1].astype(F32)
            gate = y[0]
            up = y[1]
            act[u, me_h] = (gate / (1.0 + jnp.exp(-gate)) * up).astype(BF16)
            for d in range(1, nx):
                act_x(u, d).start()
            act_p(u, 0).start()

        @pl.when(jnp.logical_and(t >= 3, t < tiles + 3))
        def _():
            u = t - 3
            for d in range(1, nx):
                act_x(u, d).wait_recv()
                act_p(u, d).start()

        @pl.when(t >= 4)
        def _():
            u = t - 4
            for d in range(nx):
                act_p(u, d).wait_recv()
            x = act[u].reshape(total_rows, tile)
            k0 = pl.multiple_of(u * tile, tile)

            def down(i, c):
                cols = pl.ds(pl.multiple_of(i * step, step), step) if width != step else slice(None)
                acc[:, cols] += jnp.dot(x, dw[pl.ds(k0, tile), cols], preferred_element_type=F32)
                return c

            lax.fori_loop(0, width // step, down, 0)

        return carry

    lax.fori_loop(0, tiles + 4, inner, 0)

    reduce_drain(pp_recv, pp_ss, pp_rs)
    pp[...] = acc[...].astype(BF16)
    chain_reduce(dn_recv, dn_ss, dn_rs, low)
    out_ref[...] = (resid[...] + low[...]).astype(BF16)
    reduce_drain(dn_recv, dn_ss, dn_rs)
    chain_drain((qall, kall, vall), qkv_ss, qkv_rs)
    chain_drain((nrm,), nrm_ss, nrm_rs)

    for d in range(1, nf):
        for c in nums(d):
            c.wait_send()
    for d in range(1, nh):
        sqs(d).wait_send()
    for d in range(1, nx):
        att_x(d).wait_send()
    for d in range(nx):
        att_p(d).wait_send()

    def drain(t, carry):
        r1_copy(t).wait_send()
        for d in range(1, nx):
            s2_copy(t, d).wait_send()
            act_x(t, d).wait_send()
        for d in range(nx):
            act_p(t, d).wait_send()
        return carry

    lax.fori_loop(0, tiles, drain, 0)


def solution(mesh):
    nf = mesh.shape["ffn"]
    nh = mesh.shape["hidden"]
    nx = nh // 2

    def shards(
        residual_in, queries, new_keys, new_values, key_cache, value_cache,
        cache_lengths, norm_gain, out_weight, gate_weight, up_weight, down_weight,
    ):
        seqs, block, kvw = key_cache.shape
        rows, qw = queries.shape
        kw = new_keys.shape[1]
        rr, width = residual_in.shape
        units = gate_weight.shape[1]
        hh = qw // HD
        tile = 512 if units % 512 == 0 else units
        tiles = units // tile
        total_rows = rows * nh
        qr = total_rows // nh

        positions = cache_lengths[:, None] + jnp.arange(DRAFT, dtype=jnp.int32)[None, :]
        steps_half = jnp.arange(HD // 2).astype(F32)
        inverse = jnp.exp(steps_half * (-2.0 * math.log(500000.0) / HD))
        angle = positions.reshape(-1).astype(F32)[:, None] * inverse[None, :]
        cos, sin = jnp.cos(angle), jnp.sin(angle)
        cos = jnp.concatenate([cos, cos], axis=1)
        sin = jnp.concatenate([-sin, sin], axis=1)
        ffn = lax.axis_index("ffn")
        slots = ffn * block + jnp.arange(block, dtype=jnp.int32)
        bias = jnp.where(slots[None, :] < cache_lengths[:, None], 0.0, -1e30).astype(F32)
        bias = bias[:, None, :]
        token = jnp.arange(GROUP * DRAFT, dtype=jnp.int32) % DRAFT
        causal = jnp.arange(DRAFT, dtype=jnp.int32)[None, :] <= token[:, None]
        dbias = jnp.where(jnp.logical_and(causal, ffn == 0), 0.0, -1e30).astype(F32)

        vm = pl.BlockSpec(memory_space=pltpu.VMEM)
        hbm = pl.BlockSpec(memory_space=pl.ANY)
        dma = pltpu.SemaphoreType.DMA
        V = pltpu.VMEM
        scratch = [
            V((2, block, kvw), BF16),
            V((2, block, kvw), BF16),
            V(out_weight.shape, BF16),
            V((SLOTS, width, tile), BF16),
            V((SLOTS, width, tile), BF16),
            V(down_weight.shape, BF16),
            V((nf, rows, qw), BF16),
            V((nf, rows, kw), BF16),
            V((nf, rows, kw), BF16),
            V((nf, rows, qw), BF16),
            V((nf - 1, rows, qw), BF16),
            V((nf, rows, hh), F32),
            V((nf - 1, rows, hh), F32),
            V((nh, rows, qw), BF16),
            V((total_rows, width), BF16),
            V((2, nf, rr, width), BF16),
            V((rr, width), F32),
            V((rr, HD), F32),
            V((nh - 1, rr, HD), F32),
            V((nf, rr, width), BF16),
            V((tiles, 2, nx, 2, qr, tile), BF16),
            V((tiles, nx, 2, qr, tile), BF16),
            V((tiles, nx - 1, 2, qr, tile), BF16),
            V((tiles, nx - 1, 2, qr, tile), BF16),
            V((tiles, nh, qr, tile), BF16),
            V((total_rows, width), F32),
            V((2, nf, rr, width), BF16),
            V((rr, width), F32),
            dma((2, 2)),
            dma((2,)),
            dma((2, SLOTS)),
            dma((3, 2, nf)), dma((3, nf)),
            dma((2, nf)), dma((2, nf)),
            dma((2 * nx,)), dma((2 * nx,)),
            dma((nf,)), dma((2, nf)),
            dma((nh,)), dma((nh,)),
            dma((1, 2, nf)), dma((1, nf)),
            dma((tiles,)), dma((tiles,)),
            dma((tiles, nx)), dma((tiles, nx)),
            dma((tiles, 2 * nx)), dma((tiles, 2 * nx)),
            dma((nf,)), dma((2, nf)),
        ]
        return pl.pallas_call(
            functools.partial(kernel, (nf, nh, seqs, tile, tiles)),
            out_shape=jax.ShapeDtypeStruct((rr, width), BF16),
            in_specs=[vm] * 9 + [hbm] * 6,
            out_specs=vm,
            scratch_shapes=scratch,
            compiler_params=pltpu.CompilerParams(
                collective_id=0, has_side_effects=True, vmem_limit_bytes=67043328
            ),
        )(
            cos, sin, bias, dbias, queries, new_keys, new_values, residual_in,
            norm_gain[None, :], key_cache, value_cache, out_weight, gate_weight,
            up_weight, down_weight,
        )

    in_specs = (
        P(("groups", "ffn"), "hidden"),
        P(("groups", "hidden"), "ffn"),
        P(("groups", "hidden"), "ffn"),
        P(("groups", "hidden"), "ffn"),
        P(("groups", "hidden"), "ffn", None),
        P(("groups", "hidden"), "ffn", None),
        P(("groups", "hidden")),
        P("hidden"),
        P("ffn", "hidden"),
        P("hidden", "ffn"),
        P("hidden", "ffn"),
        P("ffn", "hidden"),
    )
    out_specs = P(("groups", "ffn"), "hidden")
    return jax.shard_map(shards, mesh=mesh, in_specs=in_specs, out_specs=out_specs, check_vma=False)
```
